32 devices in a mesh: facet: 8 (over z, x), col: 4 (over y, core).
Axes of the slice: x: 2, y: 2, z: 4, core: 2. Of those that a mesh axis runs over, the one named last changes fastest.
Arguments:
- facets: bfloat16 [2, 8192, 1024], P(None, ('facet', 'col')), may hold values from -6 to 6
- observed: float32 [2, 32, 1024], P(None, 'col'), may hold values from -6 to 6
- uv_cells: int32 [2, 32, 1024], P(None, 'col'), may hold values from 0 to 511
- counts: int32 [32], P('col'), may hold values from 64 to 1024, as said below
Outputs:
- facet_residual: float32 [2, 8192, 1024], P(None, ('facet', 'col'))
The draws below stay inside these ranges and needn't reach their ends.
Inputs may be any that keep to these rules, and one draw needn't show every extreme that they name: Live slots of a subgrid are its first counts[s] slots; in every column some subgrid has all 1024 slots live.
All inputs are finite; a program needn't handle non-finite values.
Results may differ from the reference program's by a relative error of at most 0.008.
Values may be sent and summed in bfloat16 or wider, within the bound.
A program may use at most 64 MiB of HBM per device.

```python
import math
import jax
import jax.numpy as jnp
from jax import lax

F = 1024
S = 512
IMAGE = 65536
VIS = 1024
SUB_W = 1
NFACET = 8
SUBCOL = 8
NSUB = 32
N_FACET = 8
N_COL = 4


def draw_counts(key, part):
    key_expo, key_drop, key_full = jax.random.split(key, 3)
    exponent = jax.random.randint(key_expo, (NSUB,), 0, 4)
    ceiling = VIS // jnp.left_shift(jnp.ones((NSUB,), jnp.int32), exponent)
    lowered = jax.random.randint(key_drop, (NSUB,), 0, VIS) % (ceiling // 2 + 1)
    column_rows = NSUB // SUBCOL
    shaped = (ceiling - lowered).reshape(column_rows, SUBCOL)
    chosen = jax.random.randint(key_full, (column_rows, 1), 0, SUBCOL)
    filled = jnp.where(jnp.arange(SUBCOL, dtype=jnp.int32)[None, :] == chosen, VIS, shaped)
    return filled.reshape(NSUB).astype(jnp.int32)


def touch_ends(values, key, least, high):
    longest = values.shape.index(max(values.shape))
    spots = []
    for shift in (0, 1):
        where = [jax.random.randint(jax.random.fold_in(key, axis), (), 0, length) for axis, length in enumerate(values.shape)]
        where[longest] = (where[longest] + shift) % values.shape[longest]
        spots.append(tuple(where))
    return values.at[spots[0]].set(least).at[spots[1]].set(high)


def shard_levels(stream_key, shape, cuts, low, high):
    def one(axis_at, blocks):
        draws = jax.random.uniform(jax.random.fold_in(jax.random.fold_in(stream_key, 6), axis_at), (blocks,), jnp.float32, low / len(cuts), high / len(cuts))
        return jnp.repeat(jnp.exp(draws), shape[axis_at] // blocks).reshape((-1,) + (1,) * (len(shape) - axis_at - 1))

    gain = one(*cuts[0])
    for cut in cuts[1:]:
        gain = gain * one(*cut)
    return gain


def scatter_about(key, dims, width, limit, pieces=(), held_as=jnp.bfloat16):
    values = jax.random.normal(key, dims, jnp.float32) * width
    if len(pieces) > 0:
        values = shard_levels(key, dims, pieces, -0.22, 0.18) * values
    return jnp.clip(values, min=-limit, max=limit).astype(held_as)


def setup_inputs(seed: int = 0) -> dict:
    key_of = jax.random.split(jax.random.key(seed), 5)
    return {
        "facets": scatter_about(key_of[0], (2, NFACET * F, F), 1.0, 6.0, ((1, 32),)),
        "observed": scatter_about(key_of[1], (2, NSUB, VIS), 1.0, 6.0, ((1, 4),), jnp.float32),
        "uv_cells": touch_ends(jax.random.randint(key_of[2], (2, NSUB, VIS), 0, S), jax.random.fold_in(key_of[2], 1), 0, S - 1).astype(jnp.int32),
        "counts": draw_counts(jax.random.fold_in(key_of[4], 71), 0),
    }


def multiply_mod(left_value, right_value):
    low_part = right_value % 256
    high_part = right_value // 256
    return (left_value * low_part + left_value * high_part % IMAGE * 256) % IMAGE

def taper_values(extent):
    position = (jnp.arange(extent, dtype=jnp.int32).astype(jnp.float32) + 0.5) / extent
    return 0.6 + 0.4 * jnp.sin(math.pi * position) ** 2

def unit_table(ticks, scale, modulus):
    angle = ticks.astype(jnp.float32) * (-2.0 * math.pi / modulus)
    return jnp.stack([jnp.cos(angle) * scale, jnp.sin(angle) * scale])

def row_table(facet_id, window, spacing, extent):
    cells = facet_id // 8 * extent + jnp.arange(extent, dtype=jnp.int32)
    freqs = IMAGE // window * jnp.arange(window, dtype=jnp.int32)
    ticks = multiply_mod(cells[None, :], freqs[:, None])
    weights = taper_values(extent)[None, :] / math.sqrt(extent)
    return unit_table(ticks, weights, IMAGE).astype(jnp.bfloat16)

def column_table(facet_id, columns, window, spacing, extent):
    cells = facet_id % 8 * extent + jnp.arange(extent, dtype=jnp.int32)
    anchor = columns * (IMAGE // 4) + (29 * columns + 3) % spacing
    freqs = (anchor[:, None] + spacing * jnp.arange(window, dtype=jnp.int32)[None, :]).reshape(-1)
    ticks = multiply_mod(cells[None, :], freqs[:, None])
    weights = taper_values(extent)[None, :] / math.sqrt(extent)
    return unit_table(ticks, weights, IMAGE).astype(jnp.bfloat16)

def phase_table(facet_id, subgrid_ids, spacing, extent):
    cells = facet_id // 8 * extent + jnp.arange(extent, dtype=jnp.int32)
    anchor = subgrid_ids * (IMAGE // 64) + (37 * subgrid_ids + 5) % (IMAGE * 8 // S)
    ticks = multiply_mod(cells[None, :], anchor[:, None])
    return unit_table(ticks, 1.0, IMAGE)

def facet_windows(row_tab, phases, strip):
    phase_real = phases[0][:, :, None]
    phase_imag = phases[1][:, :, None]
    strip_real = strip[0][None].astype(jnp.float32)
    strip_imag = strip[1][None].astype(jnp.float32)
    turned_real = (phase_real * strip_real - phase_imag * strip_imag).astype(jnp.bfloat16)
    turned_imag = (phase_real * strip_imag + phase_imag * strip_real).astype(jnp.bfloat16)

    def contract(table, turned):
        return jnp.einsum('ki,sil->skl', table.astype(jnp.float32), turned.astype(jnp.float32))
    window_real = contract(row_tab[0], turned_real) - contract(row_tab[1], turned_imag)
    window_imag = contract(row_tab[0], turned_imag) + contract(row_tab[1], turned_real)
    return jnp.stack([window_real, window_imag], axis=1).astype(jnp.bfloat16)

def facet_adjoint(row_tab, phases, returned):

    def contract(table, part):
        return jnp.einsum('ki,skl->sil', table.astype(jnp.float32), part.astype(jnp.float32))
    mixed_real = contract(row_tab[0], returned[:, 0]) + contract(row_tab[1], returned[:, 1])
    mixed_imag = contract(row_tab[0], returned[:, 1]) - contract(row_tab[1], returned[:, 0])

    def weigh(phase, mixed):
        return jnp.einsum('si,sil->il', phase, mixed, precision=lax.Precision.HIGHEST)
    real_part = weigh(phases[0], mixed_real) + weigh(phases[1], mixed_imag)
    imag_part = weigh(phases[0], mixed_imag) - weigh(phases[1], mixed_real)
    return jnp.stack([real_part, imag_part])

def regrid_block(subgrid_b, observed_part, first_cells, second_cells, is_live, extent):
    cell_axis = jnp.arange(extent, dtype=jnp.int32)
    left_tab = unit_table(first_cells[:, None] * cell_axis[None, :] % extent, 1.0, extent).astype(jnp.bfloat16)
    right_tab = unit_table(second_cells[:, None] * cell_axis[None, :] % extent, 1.0, extent)

    def product(alpha, beta):
        return jnp.dot(alpha, beta, preferred_element_type=jnp.float32)
    inner_real = product(left_tab[0], subgrid_b[0]) - product(left_tab[1], subgrid_b[1])
    inner_imag = product(left_tab[0], subgrid_b[1]) + product(left_tab[1], subgrid_b[0])
    predicted_real = lax.optimization_barrier(jnp.sum(inner_real * right_tab[0] - inner_imag * right_tab[1], axis=1)) / extent
    predicted_imag = lax.optimization_barrier(jnp.sum(inner_real * right_tab[1] + inner_imag * right_tab[0], axis=1)) / extent
    resid_real = jnp.where(is_live, observed_part[0] - predicted_real, 0.0)
    resid_imag = jnp.where(is_live, observed_part[1] - predicted_imag, 0.0)
    weighted_real = (resid_real[:, None] * right_tab[0] + resid_imag[:, None] * right_tab[1]).astype(jnp.bfloat16)
    weighted_imag = (resid_imag[:, None] * right_tab[0] - resid_real[:, None] * right_tab[1]).astype(jnp.bfloat16)
    regrid_real = product(left_tab[0].T, weighted_real) + product(left_tab[1].T, weighted_imag)
    regrid_imag = product(left_tab[0].T, weighted_imag) - product(left_tab[1].T, weighted_real)
    return (regrid_real, regrid_imag)

def reference(facets, observed, uv_cells, counts):
    facet_count = N_FACET
    column_count = N_COL
    per_column = SUB_W * N_FACET
    window = S // 8
    spacing = IMAGE // F
    stacked = facets.reshape(2, facet_count, F, F).transpose(1, 0, 2, 3)
    subgrid_ids = jnp.arange(per_column, dtype=jnp.int32)
    facet_ids = jnp.arange(facet_count, dtype=jnp.int32)
    accumulated = jnp.zeros((facet_count, 2, F, F), jnp.float32)
    for column_index in range(column_count):
        columns = jnp.array([column_index], jnp.int32)

        def forward(carried, item):
            facet_id, pixels = item
            colt = column_table(facet_id, columns, window, spacing, F)
            strip_real = jnp.dot(pixels[0], colt[0].T, preferred_element_type=jnp.float32) - jnp.dot(pixels[1], colt[1].T, preferred_element_type=jnp.float32)
            strip_imag = jnp.dot(pixels[0], colt[1].T, preferred_element_type=jnp.float32) + jnp.dot(pixels[1], colt[0].T, preferred_element_type=jnp.float32)
            strip = jnp.stack([strip_real, strip_imag]).astype(jnp.bfloat16)
            windows = facet_windows(row_table(facet_id, window, spacing, F), phase_table(facet_id, subgrid_ids, spacing, F), strip)
            zero_index = jnp.zeros((), jnp.int32)
            corner = (zero_index, zero_index, (facet_id % 32 // 8 * window).astype(jnp.int32), (facet_id % 8 * window).astype(jnp.int32))
            current = lax.dynamic_slice(carried, corner, (per_column, 2, window, window))
            carried = lax.dynamic_update_slice(carried, current + windows.astype(jnp.float32), corner)
            return (carried, None)
        initial = jnp.zeros((per_column, 2, S, S), jnp.float32)
        summed, unused = lax.scan(forward, initial, (facet_ids, stacked))
        subgrid_b = summed.astype(jnp.bfloat16)
        first_row = column_index * per_column
        column_obs = observed[:, first_row:first_row + per_column].transpose(1, 0, 2)
        column_uv = uv_cells[:, first_row:first_row + per_column]
        column_counts = counts[first_row:first_row + per_column]

        def per_subgrid(item):
            grid_part, observed_part, first_cells, second_cells, live_count = item
            is_live = jnp.arange(VIS, dtype=jnp.int32) < live_count
            regrid_real, regrid_imag = regrid_block(grid_part, observed_part, first_cells, second_cells, is_live, S)
            return jnp.stack([regrid_real, regrid_imag]) * (1.0 / math.sqrt(VIS))
        regridded = lax.map(per_subgrid, (subgrid_b, column_obs, column_uv[0], column_uv[1], column_counts))

        def backward(facet_id):
            colt = column_table(facet_id, columns, window, spacing, F)
            zero_index = jnp.zeros((), jnp.int32)
            corner = (zero_index, zero_index, (facet_id % 32 // 8 * window).astype(jnp.int32), (facet_id % 8 * window).astype(jnp.int32))
            returned = lax.dynamic_slice(regridded, corner, (per_column, 2, window, window)).astype(jnp.bfloat16)
            backstrip = facet_adjoint(row_table(facet_id, window, spacing, F), phase_table(facet_id, subgrid_ids, spacing, F), returned).astype(jnp.bfloat16)
            image_real = jnp.dot(backstrip[0], colt[0], preferred_element_type=jnp.float32) + jnp.dot(backstrip[1], colt[1], preferred_element_type=jnp.float32)
            image_imag = jnp.dot(backstrip[1], colt[0], preferred_element_type=jnp.float32) - jnp.dot(backstrip[0], colt[1], preferred_element_type=jnp.float32)
            return jnp.stack([image_real, image_imag])
        accumulated = accumulated + lax.map(backward, facet_ids)
    return accumulated.transpose(1, 0, 2, 3).reshape(2, facet_count * F, F)
```

```python
import functools
import math

import jax
import jax.numpy as jnp
import numpy as np
from jax import lax
from jax.experimental import pallas as pl
from jax.experimental.pallas import tpu as pltpu
from jax.sharding import PartitionSpec as P

S = 512
IMAGE = 65536
MESH = pl.DeviceIdType.MESH
BF = jnp.bfloat16
F32 = jnp.float32


def unit(ticks):
    angle = (np.asarray(ticks, np.int64) % IMAGE) * (-2.0 * math.pi / IMAGE)
    return np.cos(angle), np.sin(angle)


def make_constants(facets, columns, per_column, extent):
    window = S // 8
    spacing = IMAGE // extent
    parts = window // 16
    cells = np.arange(extent, dtype=np.int64)
    weight = (0.6 + 0.4 * np.sin(math.pi * (cells + 0.5) / extent) ** 2) / math.sqrt(extent)
    low = np.arange(16, dtype=np.int64)
    high = 16 * np.arange(parts, dtype=np.int64)
    col = np.arange(columns, dtype=np.int64)
    vc = col * (IMAGE // 4) + (29 * col + 3) % spacing
    sub = np.arange(per_column, dtype=np.int64)
    us = sub * (IMAGE // 64) + (37 * sub + 5) % (IMAGE * 8 // S)
    grain = IMAGE // window
    rows = []
    for ticks, scale in (
        (spacing * low[:, None] * cells, 1.0),
        ((vc[:, None] + spacing * high).reshape(-1, 1) * cells, weight),
        (grain * low[:, None] * cells, 1.0),
        ((us[:, None] + grain * high).reshape(-1, 1) * cells, weight),
    ):
        real, imag = unit(ticks)
        rows += [real * scale, imag * scale]
    groups = max(facets // 8, 1)
    wide = max(columns, per_column)
    scalars = np.zeros((8 + groups, 2 * wide))
    for index in range(8):
        real, imag = unit(index * extent * vc)
        scalars[index, :columns] = real
        scalars[index, wide : wide + columns] = imag
    for index in range(groups):
        real, imag = unit(index * extent * us)
        scalars[8 + index, :per_column] = real
        scalars[8 + index, wide : wide + per_column] = imag
    return np.concatenate(rows).astype(np.float32), scalars.astype(np.float32)


def spin(value, first, second):
    half = value.shape[1] // 2
    lane = lax.broadcasted_iota(jnp.int32, value.shape, 1)
    return pltpu.roll(value, half, 1) * jnp.where(lane < half, first, second)


def cycle_kernel(
    nf, nc, x_hbm, obs, cells, counts, con, scal, back_out, tab_out,
    xbuf, tab, t2, tt, s_send, s_recv, g_send, g_recv, lt, rtr, rti, r1r, r1i, wt,
    r_send, r_recv, b_send, b_recv,
    x_sem, o_sem, sa, ra, sb, rb, sc, rc, sd, rd,
):
    f = lax.axis_index("facet")
    c = lax.axis_index("col")
    window = S // 8
    two = 2 * window
    parts = window // 16
    pc = nf
    rows = xbuf.shape[1]
    groups = max(nf // 8, 1)
    wide = max(nc, pc)
    vis = obs.shape[2]
    col_order = [d for d in range(nc - 1, 0, -1)]
    facet_order = sorted(range(1, nf), key=lambda d: -min(d, nf - d))

    barrier = pltpu.get_barrier_semaphore()
    for d in range(1, nc):
        pl.semaphore_signal(barrier, inc=1, device_id=(f, lax.rem(c + d, nc)), device_id_type=MESH)
    for d in range(1, nf):
        pl.semaphore_signal(barrier, inc=1, device_id=(lax.rem(f + d, nf), c), device_id_type=MESH)

    x_copy = pltpu.make_async_copy(x_hbm, xbuf, x_sem)
    x_copy.start()

    e1 = 32
    f0 = e1 + 2 * nc * parts
    h0 = f0 + 32
    fm = lax.rem(f, 8)

    def col_body(i, carry):
        ci = i // parts
        li = i - ci * parts
        pr, pi = scal[fm, ci], scal[fm, wide + ci]
        ar, ai = con[pl.ds(e1 + i, 1), :], con[pl.ds(e1 + nc * parts + i, 1), :]
        er, ei = ar * pr - ai * pi, ar * pi + ai * pr
        lr, lm = con[0:16, :], con[16:32, :]
        real = (lr * er - lm * ei).astype(BF)
        imag = (lr * ei + lm * er).astype(BF)
        top = pl.multiple_of(ci * two + li * 16, 16)
        low = pl.multiple_of(ci * two + window + li * 16, 16)
        tab[0, pl.ds(top, 16), :] = real
        tab[0, pl.ds(low, 16), :] = imag
        tab[1, pl.ds(top, 16), :] = -imag
        tab[1, pl.ds(low, 16), :] = real
        return carry

    lax.fori_loop(0, nc * parts, col_body, 0)
    o_copy = pltpu.make_async_copy(tab, tab_out, o_sem)
    o_copy.start()
    x_copy.wait()
    nt = (((1,), (1,)), ((), ()))
    strip = lax.dot_general(xbuf[0], tab[0], nt, preferred_element_type=F32)
    strip += lax.dot_general(xbuf[1], tab[1], nt, preferred_element_type=F32)
    for k in range(nc):
        s_send[k] = strip[:, k * two : (k + 1) * two].astype(BF)
    pl.semaphore_wait(barrier, nc - 1 + nf - 1)

    def a_copy(d):
        peer, src = lax.rem(c + d, nc), lax.rem(c + nc - d, nc)
        out = pltpu.make_async_remote_copy(
            s_send.at[peer], s_recv.at[c], sa.at[peer], ra.at[c], (f, peer), MESH
        )
        arrive = pltpu.make_async_remote_copy(
            s_send.at[peer], s_recv.at[src], sa.at[peer], ra.at[src], (f, peer), MESH
        )
        return out, arrive, src

    sends = []
    for d in col_order:
        out = a_copy(d)[0]
        out.start()
        sends.append(out)

    half = pc * window
    fg = f // 8

    def row_body(i, carry):
        j = i // parts
        ki = i - j * parts
        pr, pi = scal[8 + fg, j], scal[8 + fg, wide + j]
        ar, ai = con[pl.ds(h0 + i, 1), :], con[pl.ds(h0 + pc * parts + i, 1), :]
        er, ei = ar * pr - ai * pi, ar * pi + ai * pr
        lr, lm = con[f0 : f0 + 16, :], con[f0 + 16 : f0 + 32, :]
        at = pl.multiple_of(j * window + ki * 16, 16)
        t2[pl.ds(at, 16), :] = (lr * er - lm * ei).astype(BF)
        t2[pl.ds(pl.multiple_of(half + at, 16), 16), :] = (lr * ei + lm * er).astype(BF)
        return carry

    lax.fori_loop(0, pc * parts, row_body, 0)

    def part_product(src, block):
        start = pl.multiple_of(src * rows, rows)
        return jnp.dot(t2[:, pl.ds(start, rows)], block, preferred_element_type=F32)

    acc = part_product(c, s_send[c])
    for d in col_order[::-1]:
        unused, arrive, src = a_copy(d)
        arrive.wait_recv()
        acc += part_product(src, s_recv[src])
    win = (acc[:half] + spin(acc[half:], -1.0, 1.0)).astype(BF)
    for j in range(pc):
        g_send[j] = win[j * window : (j + 1) * window]

    def b_copy(d):
        peer, src = lax.rem(f + d, nf), lax.rem(f + nf - d, nf)
        out = pltpu.make_async_remote_copy(
            g_send.at[peer], g_recv.at[f], sb.at[peer], rb.at[f], (peer, c), MESH
        )
        arrive = pltpu.make_async_remote_copy(
            g_send.at[peer], g_recv.at[src], sb.at[peer], rb.at[src], (peer, c), MESH
        )
        return out, arrive

    for d in facet_order:
        out = b_copy(d)[0]
        out.start()
        sends.append(out)
    g_recv[f] = g_send[f]

    first = cells[0, pl.ds(f, 1), :]
    second = cells[1, pl.ds(f, 1), :]

    def wave(count, step, cell):
        index = step * lax.broadcasted_iota(jnp.int32, (count, vis), 0)
        angle = (index * cell & (S - 1)).astype(F32) * (-2.0 * math.pi / S)
        return jnp.cos(angle), jnp.sin(angle)

    l0r, l0i = wave(16, 1, first)
    l1r, l1i = wave(max(groups * parts, 8), 16, first)
    for i in range(groups * parts):
        er, ei = l1r[i : i + 1], l1i[i : i + 1]
        g, k = i // parts, i % parts
        at = g * two + k * 16
        lt[at : at + 16, :] = (l0r * er - l0i * ei).astype(BF)
        lt[at + window : at + window + 16, :] = (l0r * ei + l0i * er).astype(BF)
    m0r, m0i = wave(16, 1, second)
    r1r[...], r1i[...] = wave(S // 16, 16, second)

    def right_body(i, carry):
        er, ei = r1r[pl.ds(i, 1), :], r1i[pl.ds(i, 1), :]
        at = pl.multiple_of(i * 16, 16)
        rtr[pl.ds(at, 16), :] = m0r * er - m0i * ei
        rti[pl.ds(at, 16), :] = m0r * ei + m0i * er
        return carry

    lax.fori_loop(0, S // 16, right_body, 0)
    for i in range(2 * half // 256):
        tt[:, i * 256 : (i + 1) * 256] = t2[i * 256 : (i + 1) * 256, :].T

    for d in facet_order:
        b_copy(d)[1].wait_recv()

    pred_r = jnp.zeros((8, vis), F32)
    pred_i = jnp.zeros((8, vis), F32)
    for b in range(8):
        inner = None
        for g in range(groups):
            block = g_recv[g * 8 + b].astype(F32)
            both = jnp.concatenate([block, spin(block, -1.0, 1.0)], axis=0)
            term = jnp.dot(
                both.T.astype(BF), lt[g * two : (g + 1) * two, :], preferred_element_type=F32
            )
            inner = term if inner is None else inner + term
        ir, ii = inner[:window], inner[window:]
        rr, ri = rtr[b * window : (b + 1) * window, :], rti[b * window : (b + 1) * window, :]
        pred_r += jnp.sum((ir * rr - ii * ri).reshape(window // 8, 8, vis), axis=0)
        pred_i += jnp.sum((ir * ri + ii * rr).reshape(window // 8, 8, vis), axis=0)
    live = lax.broadcasted_iota(jnp.int32, (1, vis), 1) < counts[f]
    res_r = jnp.where(
        live, obs[0, pl.ds(f, 1), :] - jnp.sum(pred_r, axis=0, keepdims=True) / S, 0.0
    )
    res_i = jnp.where(
        live, obs[1, pl.ds(f, 1), :] - jnp.sum(pred_i, axis=0, keepdims=True) / S, 0.0
    )

    def c_copy(peer, src):
        out = pltpu.make_async_remote_copy(
            r_send.at[peer], r_recv.at[f], sc.at[peer], rc.at[f], (peer, c), MESH
        )
        arrive = pltpu.make_async_remote_copy(
            r_send.at[peer], r_recv.at[src], sc.at[peer], rc.at[src], (peer, c), MESH
        )
        return out, arrive

    scale = 1.0 / math.sqrt(vis)
    for b in range(0, 8, 2):
        for h in range(2):
            at = (b + h) * window
            rr, ri = rtr[at : at + window, :], rti[at : at + window, :]
            wt[2 * at : 2 * at + window, :] = (res_r * rr + res_i * ri).astype(BF)
            wt[2 * at + window : 2 * at + two, :] = (res_i * rr - res_r * ri).astype(BF)
        grid = lax.dot_general(
            lt[...], wt[b * two : (b + 2) * two, :], nt, preferred_element_type=F32
        )
        for g in range(groups):
            for h in range(2):
                u = grid[g * two : g * two + window, h * two : (h + 1) * two]
                v = grid[g * two + window : (g + 1) * two, h * two : (h + 1) * two]
                r_send[g * 8 + b + h] = ((u + spin(v, 1.0, -1.0)) * scale).astype(BF)
    for d in facet_order:
        out = c_copy(lax.rem(f + d, nf), lax.rem(f + nf - d, nf))[0]
        out.start()
        sends.append(out)
    r_recv[f] = r_send[f]
    for d in facet_order:
        c_copy(lax.rem(f + d, nf), lax.rem(f + nf - d, nf))[1].wait_recv()

    ret = r_recv[...].reshape(half, two)
    other = spin(ret.astype(F32), 1.0, -1.0).astype(BF)
    strip = jnp.dot(tt[:, :half], ret, preferred_element_type=F32)
    strip += jnp.dot(tt[:, half:], other, preferred_element_type=F32)
    for k in range(nc):
        b_send[k] = strip[k * rows : (k + 1) * rows].astype(BF)

    def d_copy(d):
        peer, src = lax.rem(c + d, nc), lax.rem(c + nc - d, nc)
        out = pltpu.make_async_remote_copy(
            b_send.at[peer], b_recv.at[c], sd.at[peer], rd.at[c], (f, peer), MESH
        )
        arrive = pltpu.make_async_remote_copy(
            b_send.at[peer], b_recv.at[src], sd.at[peer], rd.at[src], (f, peer), MESH
        )
        return out, arrive

    for d in col_order:
        out = d_copy(d)[0]
        out.start()
        sends.append(out)
    b_recv[c] = b_send[c]
    o_copy.wait()
    for d in col_order:
        d_copy(d)[1].wait_recv()
    back_out[...] = b_recv[...]
    for out in sends:
        out.wait_send()


def image_kernel(nc, back, tab, out):
    strip = jnp.concatenate([back[k] for k in range(nc)], axis=1)
    out[0] = jnp.dot(strip, tab[0], preferred_element_type=F32)
    out[1] = jnp.dot(strip, tab[1], preferred_element_type=F32)


def solution(mesh):
    nf, nc = mesh.shape["facet"], mesh.shape["col"]

    def on_device(facets, observed, uv_cells, counts):
        rows, extent = facets.shape[1:]
        vis = observed.shape[2]
        pc = counts.shape[0]
        window = S // 8
        two = 2 * window
        groups = nf // 8
        assert pc == nf and nf % 8 == 0 and nf <= 32
        con, scal = make_constants(nf, nc, pc, extent)
        vmem = pl.BlockSpec(memory_space=pltpu.VMEM)
        smem = pl.BlockSpec(memory_space=pltpu.SMEM)
        hbm = pl.BlockSpec(memory_space=pl.ANY)
        dma = pltpu.SemaphoreType.DMA
        back, tab = pl.pallas_call(
            functools.partial(cycle_kernel, nf, nc),
            out_shape=(
                jax.ShapeDtypeStruct((nc, rows, two), BF),
                jax.ShapeDtypeStruct((2, nc * two, extent), BF),
            ),
            in_specs=[hbm, vmem, vmem, smem, vmem, smem],
            out_specs=(vmem, hbm),
            scratch_shapes=[
                pltpu.VMEM((2, rows, extent), BF),
                pltpu.VMEM((2, nc * two, extent), BF),
                pltpu.VMEM((2 * pc * window, extent), BF),
                pltpu.VMEM((extent, 2 * pc * window), BF),
                pltpu.VMEM((nc, rows, two), BF),
                pltpu.VMEM((nc, rows, two), BF),
                pltpu.VMEM((pc, window, two), BF),
                pltpu.VMEM((nf, window, two), BF),
                pltpu.VMEM((groups * two, vis), BF),
                pltpu.VMEM((S, vis), F32),
                pltpu.VMEM((S, vis), F32),
                pltpu.VMEM((S // 16, vis), F32),
                pltpu.VMEM((S // 16, vis), F32),
                pltpu.VMEM((2 * S, vis), BF),
                pltpu.VMEM((nf, window, two), BF),
                pltpu.VMEM((pc, window, two), BF),
                pltpu.VMEM((nc, rows, two), BF),
                pltpu.VMEM((nc, rows, two), BF),
                dma, dma,
                dma((nc,)), dma((nc,)), dma((nf,)), dma((nf,)),
                dma((nf,)), dma((nf,)), dma((nc,)), dma((nc,)),
            ],
            compiler_params=pltpu.CompilerParams(collective_id=0, has_side_effects=True),
            name="cycle",
        )(facets, observed, uv_cells, counts, jnp.asarray(con), jnp.asarray(scal))
        tile = 256
        return pl.pallas_call(
            functools.partial(image_kernel, nc),
            grid=(extent // tile,),
            out_shape=jax.ShapeDtypeStruct((2, rows, extent), F32),
            in_specs=[
                pl.BlockSpec((nc, rows, two), lambda i: (0, 0, 0)),
                pl.BlockSpec((2, nc * two, tile), lambda i: (0, 0, i)),
            ],
            out_specs=pl.BlockSpec((2, rows, tile), lambda i: (0, 0, i)),
            name="image",
        )(back, tab)

    return jax.shard_map(
        on_device,
        mesh=mesh,
        in_specs=(
            P(None, ("facet", "col"), None),
            P(None, "col", None),
            P(None, "col", None),
            P("col"),
        ),
        out_specs=P(None, ("facet", "col"), None),
        check_vma=False,
    )
```

```python
import functools
import math

import jax
import jax.numpy as jnp
import numpy as np
from jax import lax
from jax.experimental import pallas as pl
from jax.experimental.pallas import tpu as pltpu
from jax.sharding import PartitionSpec as P

S = 512
IMAGE = 65536
MESH = pl.DeviceIdType.MESH
BF = jnp.bfloat16
F32 = jnp.float32


def unit(ticks):
    angle = (np.asarray(ticks, np.int64) % IMAGE) * (-2.0 * math.pi / IMAGE)
    return np.cos(angle), np.sin(angle)


def make_constants(facets, columns, per_column, extent):
    window = S // 8
    spacing = IMAGE // extent
    parts = window // 16
    cells = np.arange(extent, dtype=np.int64)
    weight = (0.6 + 0.4 * np.sin(math.pi * (cells + 0.5) / extent) ** 2) / math.sqrt(extent)
    low = np.arange(16, dtype=np.int64)
    high = 16 * np.arange(parts, dtype=np.int64)
    col = np.arange(columns, dtype=np.int64)
    vc = col * (IMAGE // 4) + (29 * col + 3) % spacing
    sub = np.arange(per_column, dtype=np.int64)
    us = sub * (IMAGE // 64) + (37 * sub + 5) % (IMAGE * 8 // S)
    grain = IMAGE // window
    rows = []
    for ticks, scale in (
        (spacing * low[:, None] * cells, 1.0),
        ((vc[:, None] + spacing * high).reshape(-1, 1) * cells, weight),
        (grain * low[:, None] * cells, 1.0),
        ((us[:, None] + grain * high).reshape(-1, 1) * cells, weight),
    ):
        real, imag = unit(ticks)
        rows += [real * scale, imag * scale]
    groups = max(facets // 8, 1)
    wide = max(columns, per_column)
    scalars = np.zeros((8 + groups, 2 * wide))
    for index in range(8):
        real, imag = unit(index * extent * vc)
        scalars[index, :columns] = real
        scalars[index, wide : wide + columns] = imag
    for index in range(groups):
        real, imag = unit(index * extent * us)
        scalars[8 + index, :per_column] = real
        scalars[8 + index, wide : wide + per_column] = imag
    return np.concatenate(rows).astype(np.float32), scalars.astype(np.float32)


def spin(value, first, second):
    half = value.shape[1] // 2
    lane = lax.broadcasted_iota(jnp.int32, value.shape, 1)
    return pltpu.roll(value, half, 1) * jnp.where(lane < half, first, second)


def cycle_kernel(
    nf, nc, xbuf, obs, cells, counts, con, scal, back_out, tab,
    t2, tt, s_send, s_recv, g_send, g_recv, lt, rtr, rti, r1r, r1i, wt,
    r_send, r_recv, b_send, b_recv,
    sa, ra, sb, rb, sc, rc, sd, rd,
):
    f = lax.axis_index("facet")
    c = lax.axis_index("col")
    window = S // 8
    two = 2 * window
    parts = window // 16
    pc = nf
    rows = xbuf.shape[1]
    groups = nf // 8
    wide = max(nc, pc)
    vis = obs.shape[2]
    if nc % 2:
        col_steps = [(d, 0) for d in range(1, nc)]
    else:
        col_steps = [(d, k) for d in range(nc // 2 - 1, -1, -1) for k in range(2) if d or k]

    def col_at(step, sign):
        if nc % 2:
            return lax.rem(c + nc + sign * step[0], nc)
        top = lax.rem(c // 2 + nc // 2 + sign * step[0], nc // 2)
        return 2 * top + lax.rem(c + step[1], 2)

    def pair_at(q):
        return lax.rem(f // 2 + q, 4)

    def facet_link(src_buf, dst_buf, send, recv, peer, slot):
        return pltpu.make_async_remote_copy(
            src_buf.at[peer], dst_buf.at[slot], send.at[peer], recv.at[slot], (peer, c), MESH
        )

    def col_link(src_buf, dst_buf, send, recv, peer, slot):
        return pltpu.make_async_remote_copy(
            src_buf.at[peer], dst_buf.at[slot], send.at[peer], recv.at[slot], (f, peer), MESH
        )

    barrier = pltpu.get_barrier_semaphore()
    for d in range(1, nc):
        pl.semaphore_signal(barrier, inc=1, device_id=(f, lax.rem(c + d, nc)), device_id_type=MESH)
    for d in range(1, nf):
        pl.semaphore_signal(barrier, inc=1, device_id=(lax.rem(f + d, nf), c), device_id_type=MESH)

    e1 = 32
    f0 = e1 + 2 * nc * parts
    h0 = f0 + 32
    nt = (((1,), (1,)), ((), ()))
    fm = lax.rem(f, 8)

    def column_table(cp):
        pr, pi = scal[fm, cp], scal[fm, wide + cp]
        lr, lm = con[0:16, :], con[16:32, :]
        for li in range(parts):
            i = cp * parts + li
            ar, ai = con[pl.ds(e1 + i, 1), :], con[pl.ds(e1 + nc * parts + i, 1), :]
            er, ei = ar * pr - ai * pi, ar * pi + ai * pr
            real = (lr * er - lm * ei).astype(BF)
            imag = (lr * ei + lm * er).astype(BF)
            top = pl.multiple_of(cp * two + li * 16, 16)
            low = pl.multiple_of(cp * two + window + li * 16, 16)
            tab[0, pl.ds(top, 16), :] = real
            tab[0, pl.ds(low, 16), :] = imag
            tab[1, pl.ds(top, 16), :] = -imag
            tab[1, pl.ds(low, 16), :] = real

    def column_strip(cp):
        at = pl.multiple_of(cp * two, two)
        strip = lax.dot_general(xbuf[0], tab[0, pl.ds(at, two), :], nt, preferred_element_type=F32)
        strip += lax.dot_general(xbuf[1], tab[1, pl.ds(at, two), :], nt, preferred_element_type=F32)
        s_send[cp] = strip.astype(BF)

    for n, step in enumerate(col_steps):
        peer = col_at(step, 1)
        column_table(peer)
        column_strip(peer)
        if n == 0:
            pl.semaphore_wait(barrier, nc - 1 + nf - 1)
        col_link(s_send, s_recv, sa, ra, peer, c).start()
    column_table(c)
    column_strip(c)

    half = pc * window
    fg = f // 8

    def row_body(i, carry):
        j = i // parts
        ki = i - j * parts
        pr, pi = scal[8 + fg, j], scal[8 + fg, wide + j]
        ar, ai = con[pl.ds(h0 + i, 1), :], con[pl.ds(h0 + pc * parts + i, 1), :]
        er, ei = ar * pr - ai * pi, ar * pi + ai * pr
        lr, lm = con[f0 : f0 + 16, :], con[f0 + 16 : f0 + 32, :]
        at = pl.multiple_of(j * window + ki * 16, 16)
        t2[pl.ds(at, 16), :] = (lr * er - lm * ei).astype(BF)
        t2[pl.ds(pl.multiple_of(half + at, 16), 16), :] = (lr * ei + lm * er).astype(BF)
        return carry

    lax.fori_loop(0, pc * parts, row_body, 0)

    def part_product(src, block):
        start = pl.multiple_of(src * rows, rows)
        return jnp.dot(t2[:, pl.ds(start, rows)], block, preferred_element_type=F32)

    acc = part_product(c, s_send[c])
    for step in col_steps[::-1]:
        src = col_at(step, -1)
        col_link(s_send, s_recv, sa, ra, src, src).wait_recv()
        acc += part_product(src, s_recv[src])
    win = (acc[:half] + spin(acc[half:], -1.0, 1.0)).astype(BF)
    for j in range(pc):
        g_send[j] = win[j * window : (j + 1) * window]

    def each_facet(q, act):
        pair = pair_at(q)
        for g in range(groups):
            for h in range(2):
                index = g * 8 + 2 * pair + h
                if q == 0:
                    pl.when(index != f)(functools.partial(act, index))
                else:
                    act(index)

    def send_window(index):
        facet_link(g_send, g_recv, sb, rb, index, f).start()

    def take_window(index):
        facet_link(g_send, g_recv, sb, rb, index, index).wait_recv()

    def send_back(index):
        facet_link(r_send, r_recv, sc, rc, index, f).start()

    def take_back(index):
        facet_link(r_send, r_recv, sc, rc, index, index).wait_recv()

    far_first = (2, 3, 1, 0)
    for q in far_first:
        each_facet(q, send_window)
    g_recv[f] = g_send[f]

    first = cells[0, pl.ds(f, 1), :]
    second = cells[1, pl.ds(f, 1), :]

    def wave(count, step, cell):
        index = step * lax.broadcasted_iota(jnp.int32, (count, vis), 0)
        angle = (index * cell & (S - 1)).astype(F32) * (-2.0 * math.pi / S)
        return jnp.cos(angle), jnp.sin(angle)

    l0r, l0i = wave(16, 1, first)
    l1r, l1i = wave(max(groups * parts, 8), 16, first)
    for i in range(groups * parts):
        er, ei = l1r[i : i + 1], l1i[i : i + 1]
        g, k = i // parts, i % parts
        at = g * two + k * 16
        lt[at : at + 16, :] = (l0r * er - l0i * ei).astype(BF)
        lt[at + window : at + window + 16, :] = (l0r * ei + l0i * er).astype(BF)
    m0r, m0i = wave(16, 1, second)
    r1r[...], r1i[...] = wave(S // 16, 16, second)

    def right_body(i, carry):
        er, ei = r1r[pl.ds(i, 1), :], r1i[pl.ds(i, 1), :]
        at = pl.multiple_of(i * 16, 16)
        rtr[pl.ds(at, 16), :] = m0r * er - m0i * ei
        rti[pl.ds(at, 16), :] = m0r * ei + m0i * er
        return carry

    lax.fori_loop(0, S // 16, right_body, 0)

    pred_r = jnp.zeros((8, vis), F32)
    pred_i = jnp.zeros((8, vis), F32)
    for q in far_first[::-1]:
        each_facet(q, take_window)
        for h in range(2):
            b = 2 * pair_at(q) + h
            inner = None
            for g in range(groups):
                block = g_recv[g * 8 + b].astype(F32)
                both = jnp.concatenate([block, spin(block, -1.0, 1.0)], axis=0)
                term = jnp.dot(
                    both.T.astype(BF), lt[g * two : (g + 1) * two, :], preferred_element_type=F32
                )
                inner = term if inner is None else inner + term
            ir, ii = inner[:window], inner[window:]
            at = pl.multiple_of(b * window, window)
            rr, ri = rtr[pl.ds(at, window), :], rti[pl.ds(at, window), :]
            pred_r += jnp.sum((ir * rr - ii * ri).reshape(window // 8, 8, vis), axis=0)
            pred_i += jnp.sum((ir * ri + ii * rr).reshape(window // 8, 8, vis), axis=0)
    live = lax.broadcasted_iota(jnp.int32, (1, vis), 1) < counts[f]
    res_r = jnp.where(
        live, obs[0, pl.ds(f, 1), :] - jnp.sum(pred_r, axis=0, keepdims=True) / S, 0.0
    )
    res_i = jnp.where(
        live, obs[1, pl.ds(f, 1), :] - jnp.sum(pred_i, axis=0, keepdims=True) / S, 0.0
    )

    scale = 1.0 / math.sqrt(vis)
    for n, q in enumerate(far_first):
        base = n * 2 * two
        for h in range(2):
            at = pl.multiple_of((2 * pair_at(q) + h) * window, window)
            rr, ri = rtr[pl.ds(at, window), :], rti[pl.ds(at, window), :]
            low = base + h * two
            wt[low : low + window, :] = (res_r * rr + res_i * ri).astype(BF)
            wt[low + window : low + two, :] = (res_i * rr - res_r * ri).astype(BF)
        grid = lax.dot_general(
            lt[...], wt[base : base + 2 * two, :], nt, preferred_element_type=F32
        )
        for g in range(groups):
            for h in range(2):
                u = grid[g * two : g * two + window, h * two : (h + 1) * two]
                v = grid[g * two + window : (g + 1) * two, h * two : (h + 1) * two]
                index = g * 8 + 2 * pair_at(q) + h
                r_send[index] = ((u + spin(v, 1.0, -1.0)) * scale).astype(BF)
        each_facet(q, send_back)
    r_recv[f] = r_send[f]
    for i in range(2 * half // 256):
        tt[:, i * 256 : (i + 1) * 256] = t2[i * 256 : (i + 1) * 256, :].T
    for q in far_first[::-1]:
        each_facet(q, take_back)

    ret = r_recv[...].reshape(half, two)
    other = spin(ret.astype(F32), 1.0, -1.0).astype(BF)

    def back_strip(cp):
        at = pl.multiple_of(cp * rows, rows)
        strip = jnp.dot(tt[pl.ds(at, rows), :half], ret, preferred_element_type=F32)
        strip += jnp.dot(tt[pl.ds(at, rows), half:], other, preferred_element_type=F32)
        b_send[cp] = strip.astype(BF)

    for step in col_steps:
        peer = col_at(step, 1)
        back_strip(peer)
        col_link(b_send, b_recv, sd, rd, peer, c).start()
    back_strip(c)
    back_out[c] = b_send[c]
    for step in col_steps[::-1]:
        src = col_at(step, -1)
        col_link(b_send, b_recv, sd, rd, src, src).wait_recv()
        back_out[src] = b_recv[src]
    for step in col_steps:
        peer = col_at(step, 1)
        col_link(s_send, s_recv, sa, ra, peer, c).wait_send()
        col_link(b_send, b_recv, sd, rd, peer, c).wait_send()
    for d in range(1, nf):
        peer = lax.rem(f + d, nf)
        facet_link(g_send, g_recv, sb, rb, peer, f).wait_send()
        facet_link(r_send, r_recv, sc, rc, peer, f).wait_send()


def image_kernel(nc, back, tab, out, buf, sem):
    tiles, tile = buf.shape[0], buf.shape[3]
    strip = jnp.concatenate([back[k] for k in range(nc)], axis=1)
    stores = []
    for t in range(tiles):
        for part in range(2):
            piece = tab[part, :, t * tile : (t + 1) * tile]
            buf[t, part] = jnp.dot(strip, piece, preferred_element_type=F32)
        store = pltpu.make_async_copy(
            buf.at[t], out.at[:, :, t * tile : (t + 1) * tile], sem.at[t]
        )
        store.start()
        stores.append(store)
    for store in stores:
        store.wait()


def solution(mesh):
    nf, nc = mesh.shape["facet"], mesh.shape["col"]

    def on_device(facets, observed, uv_cells, counts):
        rows, extent = facets.shape[1:]
        vis = observed.shape[2]
        pc = counts.shape[0]
        window = S // 8
        two = 2 * window
        groups = nf // 8
        assert pc == nf and nf % 8 == 0 and nf <= 32
        con, scal = make_constants(nf, nc, pc, extent)
        vmem = pl.BlockSpec(memory_space=pltpu.VMEM)
        smem = pl.BlockSpec(memory_space=pltpu.SMEM)
        hbm = pl.BlockSpec(memory_space=pltpu.HBM)
        dma = pltpu.SemaphoreType.DMA
        back, tab = pl.pallas_call(
            functools.partial(cycle_kernel, nf, nc),
            out_shape=(
                jax.ShapeDtypeStruct((nc, rows, two), BF),
                jax.ShapeDtypeStruct((2, nc * two, extent), BF),
            ),
            in_specs=[vmem, vmem, vmem, smem, vmem, smem],
            out_specs=(vmem, vmem),
            scratch_shapes=[
                pltpu.VMEM((2 * pc * window, extent), BF),
                pltpu.VMEM((extent, 2 * pc * window), BF),
                pltpu.VMEM((nc, rows, two), BF),
                pltpu.VMEM((nc, rows, two), BF),
                pltpu.VMEM((pc, window, two), BF),
                pltpu.VMEM((nf, window, two), BF),
                pltpu.VMEM((groups * two, vis), BF),
                pltpu.VMEM((S, vis), F32),
                pltpu.VMEM((S, vis), F32),
                pltpu.VMEM((S // 16, vis), F32),
                pltpu.VMEM((S // 16, vis), F32),
                pltpu.VMEM((2 * S, vis), BF),
                pltpu.VMEM((nf, window, two), BF),
                pltpu.VMEM((pc, window, two), BF),
                pltpu.VMEM((nc, rows, two), BF),
                pltpu.VMEM((nc, rows, two), BF),
                dma((nc,)), dma((nc,)), dma((nf,)), dma((nf,)),
                dma((nf,)), dma((nf,)), dma((nc,)), dma((nc,)),
            ],
            compiler_params=pltpu.CompilerParams(
                collective_id=0, has_side_effects=True, vmem_limit_bytes=44 * 2**20
            ),
            name="cycle",
        )(facets, observed, uv_cells, counts, jnp.asarray(con), jnp.asarray(scal))
        tile = 256
        return pl.pallas_call(
            functools.partial(image_kernel, nc),
            out_shape=jax.ShapeDtypeStruct((2, rows, extent), F32),
            in_specs=[vmem, vmem],
            out_specs=hbm,
            scratch_shapes=[
                pltpu.VMEM((extent // tile, 2, rows, tile), F32),
                dma((extent // tile,)),
            ],
            compiler_params=pltpu.CompilerParams(vmem_limit_bytes=16 * 2**20),
            name="image",
        )(back, tab)

    return jax.shard_map(
        on_device,
        mesh=mesh,
        in_specs=(
            P(None, ("facet", "col"), None),
            P(None, "col", None),
            P(None, "col", None),
            P("col"),
        ),
        out_specs=P(None, ("facet", "col"), None),
        check_vma=False,
    )
```

```python
import functools
import math

import jax
import jax.numpy as jnp
import numpy as np
from jax import lax
from jax.experimental import pallas as pl
from jax.experimental.pallas import tpu as pltpu
from jax.sharding import PartitionSpec as P

S = 512
IMAGE = 65536
MESH = pl.DeviceIdType.MESH
BF = jnp.bfloat16
F32 = jnp.float32


def unit(ticks):
    angle = (np.asarray(ticks, np.int64) % IMAGE) * (-2.0 * math.pi / IMAGE)
    return np.cos(angle), np.sin(angle)


def make_constants(facets, columns, per_column, extent):
    window = S // 8
    spacing = IMAGE // extent
    parts = window // 16
    cells = np.arange(extent, dtype=np.int64)
    weight = (0.6 + 0.4 * np.sin(math.pi * (cells + 0.5) / extent) ** 2) / math.sqrt(extent)
    low = np.arange(16, dtype=np.int64)
    high = 16 * np.arange(parts, dtype=np.int64)
    col = np.arange(columns, dtype=np.int64)
    vc = col * (IMAGE // 4) + (29 * col + 3) % spacing
    sub = np.arange(per_column, dtype=np.int64)
    us = sub * (IMAGE // 64) + (37 * sub + 5) % (IMAGE * 8 // S)
    grain = IMAGE // window
    rows = []
    for ticks, scale in (
        (spacing * low[:, None] * cells, 1.0),
        ((vc[:, None] + spacing * high).reshape(-1, 1) * cells, weight),
        (grain * low[:, None] * cells, 1.0),
        ((us[:, None] + grain * high).reshape(-1, 1) * cells, weight),
    ):
        real, imag = unit(ticks)
        rows += [real * scale, imag * scale]
    groups = max(facets // 8, 1)
    wide = max(columns, per_column)
    scalars = np.zeros((8 + groups, 2 * wide))
    for index in range(8):
        real, imag = unit(index * extent * vc)
        scalars[index, :columns] = real
        scalars[index, wide : wide + columns] = imag
    for index in range(groups):
        real, imag = unit(index * extent * us)
        scalars[8 + index, :per_column] = real
        scalars[8 + index, wide : wide + per_column] = imag
    return np.concatenate(rows).astype(np.float32), scalars.astype(np.float32)


def spin(value, first, second):
    half = value.shape[1] // 2
    lane = lax.broadcasted_iota(jnp.int32, value.shape, 1)
    return pltpu.roll(value, half, 1) * jnp.where(lane < half, first, second)


def cycle_kernel(
    nf, nc, x_hbm, obs_hbm, cells_hbm, counts, con_hbm, scal, back_out, tab,
    xbuf, obs, cells, con, t2, tt, s_send, s_recv, g_send, g_recv, lt, rtr, rti, r1r, r1i, wt,
    r_send, r_recv, b_send, b_recv,
    in_sem, sa, ra, sb, rb, sc, rc, sd, rd,
):
    f = lax.axis_index("facet")
    c = lax.axis_index("col")
    window = S // 8
    two = 2 * window
    parts = window // 16
    pc = nf
    rows = xbuf.shape[1]
    groups = nf // 8
    wide = max(nc, pc)
    vis = obs.shape[2]
    if nc % 2:
        col_steps = [(d, 0) for d in range(1, nc)]
    else:
        col_steps = [(d, k) for d in range(nc // 2 - 1, -1, -1) for k in range(2) if d or k]

    def col_at(step, sign):
        if nc % 2:
            return lax.rem(c + nc + sign * step[0], nc)
        top = lax.rem(c // 2 + nc // 2 + sign * step[0], nc // 2)
        return 2 * top + lax.rem(c + step[1], 2)

    def pair_at(q):
        return lax.rem(f // 2 + q, 4)

    def facet_link(src_buf, dst_buf, send, recv, peer, slot):
        return pltpu.make_async_remote_copy(
            src_buf.at[peer], dst_buf.at[slot], send.at[peer], recv.at[slot], (peer, c), MESH
        )

    def col_link(src_buf, dst_buf, send, recv, peer, slot):
        return pltpu.make_async_remote_copy(
            src_buf.at[peer], dst_buf.at[slot], send.at[peer], recv.at[slot], (f, peer), MESH
        )

    barrier = pltpu.get_barrier_semaphore()
    for d in range(1, nc):
        pl.semaphore_signal(barrier, inc=1, device_id=(f, lax.rem(c + d, nc)), device_id_type=MESH)
    for d in range(1, nf):
        pl.semaphore_signal(barrier, inc=1, device_id=(lax.rem(f + d, nf), c), device_id_type=MESH)

    e1 = 32
    f0 = e1 + 2 * nc * parts
    h0 = f0 + 32
    last = con.shape[0]
    loads = [
        pltpu.make_async_copy(con_hbm.at[0:f0], con.at[0:f0], in_sem.at[0]),
        pltpu.make_async_copy(x_hbm, xbuf, in_sem.at[1]),
        pltpu.make_async_copy(con_hbm.at[f0:last], con.at[f0:last], in_sem.at[2]),
        pltpu.make_async_copy(obs_hbm, obs, in_sem.at[3]),
        pltpu.make_async_copy(cells_hbm, cells, in_sem.at[4]),
    ]
    for load in loads:
        load.start()
    nt = (((1,), (1,)), ((), ()))
    fm = lax.rem(f, 8)

    def column_table(cp):
        pr, pi = scal[fm, cp], scal[fm, wide + cp]
        lr, lm = con[0:16, :], con[16:32, :]
        for li in range(parts):
            i = cp * parts + li
            ar, ai = con[pl.ds(e1 + i, 1), :], con[pl.ds(e1 + nc * parts + i, 1), :]
            er, ei = ar * pr - ai * pi, ar * pi + ai * pr
            real = (lr * er - lm * ei).astype(BF)
            imag = (lr * ei + lm * er).astype(BF)
            top = pl.multiple_of(cp * two + li * 16, 16)
            low = pl.multiple_of(cp * two + window + li * 16, 16)
            tab[0, pl.ds(top, 16), :] = real
            tab[0, pl.ds(low, 16), :] = imag
            tab[1, pl.ds(top, 16), :] = -imag
            tab[1, pl.ds(low, 16), :] = real

    def column_strip(cp):
        at = pl.multiple_of(cp * two, two)
        strip = lax.dot_general(xbuf[0], tab[0, pl.ds(at, two), :], nt, preferred_element_type=F32)
        strip += lax.dot_general(xbuf[1], tab[1, pl.ds(at, two), :], nt, preferred_element_type=F32)
        s_send[cp] = strip.astype(BF)

    loads[0].wait()
    for n, step in enumerate(col_steps):
        peer = col_at(step, 1)
        column_table(peer)
        if n == 0:
            loads[1].wait()
        column_strip(peer)
        if n == 0:
            pl.semaphore_wait(barrier, nc - 1 + nf - 1)
        col_link(s_send, s_recv, sa, ra, peer, c).start()
    column_table(c)
    column_strip(c)

    half = pc * window
    fg = f // 8

    loads[2].wait()

    def row_body(i, carry):
        j = i // parts
        ki = i - j * parts
        pr, pi = scal[8 + fg, j], scal[8 + fg, wide + j]
        ar, ai = con[pl.ds(h0 + i, 1), :], con[pl.ds(h0 + pc * parts + i, 1), :]
        er, ei = ar * pr - ai * pi, ar * pi + ai * pr
        lr, lm = con[f0 : f0 + 16, :], con[f0 + 16 : f0 + 32, :]
        at = pl.multiple_of(j * window + ki * 16, 16)
        t2[pl.ds(at, 16), :] = (lr * er - lm * ei).astype(BF)
        t2[pl.ds(pl.multiple_of(half + at, 16), 16), :] = (lr * ei + lm * er).astype(BF)
        return carry

    lax.fori_loop(0, pc * parts, row_body, 0)

    def part_product(src, block):
        start = pl.multiple_of(src * rows, rows)
        return jnp.dot(t2[:, pl.ds(start, rows)], block, preferred_element_type=F32)

    acc = part_product(c, s_send[c])
    for step in col_steps[::-1]:
        src = col_at(step, -1)
        col_link(s_send, s_recv, sa, ra, src, src).wait_recv()
        acc += part_product(src, s_recv[src])
    win = (acc[:half] + spin(acc[half:], -1.0, 1.0)).astype(BF)
    for j in range(pc):
        g_send[j] = win[j * window : (j + 1) * window]

    def each_facet(q, act):
        pair = pair_at(q)
        for g in range(groups):
            for h in range(2):
                index = g * 8 + 2 * pair + h
                if q == 0:
                    pl.when(index != f)(functools.partial(act, index))
                else:
                    act(index)

    def send_window(index):
        facet_link(g_send, g_recv, sb, rb, index, f).start()

    def take_window(index):
        facet_link(g_send, g_recv, sb, rb, index, index).wait_recv()

    def send_back(index):
        facet_link(r_send, r_recv, sc, rc, index, f).start()

    def take_back(index):
        facet_link(r_send, r_recv, sc, rc, index, index).wait_recv()

    far_first = (2, 3, 1, 0)
    for q in far_first:
        each_facet(q, send_window)
    g_recv[f] = g_send[f]

    loads[3].wait()
    loads[4].wait()
    first = cells[0, pl.ds(f, 1), :]
    second = cells[1, pl.ds(f, 1), :]

    def wave(count, step, cell):
        index = step * lax.broadcasted_iota(jnp.int32, (count, vis), 0)
        angle = (index * cell & (S - 1)).astype(F32) * (-2.0 * math.pi / S)
        return jnp.cos(angle), jnp.sin(angle)

    l0r, l0i = wave(16, 1, first)
    l1r, l1i = wave(max(groups * parts, 8), 16, first)
    for i in range(groups * parts):
        er, ei = l1r[i : i + 1], l1i[i : i + 1]
        g, k = i // parts, i % parts
        at = g * two + k * 16
        lt[at : at + 16, :] = (l0r * er - l0i * ei).astype(BF)
        lt[at + window : at + window + 16, :] = (l0r * ei + l0i * er).astype(BF)
    m0r, m0i = wave(16, 1, second)
    r1r[...], r1i[...] = wave(S // 16, 16, second)

    def right_body(i, carry):
        er, ei = r1r[pl.ds(i, 1), :], r1i[pl.ds(i, 1), :]
        at = pl.multiple_of(i * 16, 16)
        rtr[pl.ds(at, 16), :] = m0r * er - m0i * ei
        rti[pl.ds(at, 16), :] = m0r * ei + m0i * er
        return carry

    lax.fori_loop(0, S // 16, right_body, 0)

    pred_r = jnp.zeros((8, vis), F32)
    pred_i = jnp.zeros((8, vis), F32)
    for q in far_first[::-1]:
        each_facet(q, take_window)
        for h in range(2):
            b = 2 * pair_at(q) + h
            inner = None
            for g in range(groups):
                block = g_recv[g * 8 + b].astype(F32)
                both = jnp.concatenate([block, spin(block, -1.0, 1.0)], axis=0)
                term = jnp.dot(
                    both.T.astype(BF), lt[g * two : (g + 1) * two, :], preferred_element_type=F32
                )
                inner = term if inner is None else inner + term
            ir, ii = inner[:window], inner[window:]
            at = pl.multiple_of(b * window, window)
            rr, ri = rtr[pl.ds(at, window), :], rti[pl.ds(at, window), :]
            pred_r += jnp.sum((ir * rr - ii * ri).reshape(window // 8, 8, vis), axis=0)
            pred_i += jnp.sum((ir * ri + ii * rr).reshape(window // 8, 8, vis), axis=0)
    live = lax.broadcasted_iota(jnp.int32, (1, vis), 1) < counts[f]
    res_r = jnp.where(
        live, obs[0, pl.ds(f, 1), :] - jnp.sum(pred_r, axis=0, keepdims=True) / S, 0.0
    )
    res_i = jnp.where(
        live, obs[1, pl.ds(f, 1), :] - jnp.sum(pred_i, axis=0, keepdims=True) / S, 0.0
    )

    scale = 1.0 / math.sqrt(vis)
    for n, q in enumerate(far_first):
        base = n * 2 * two
        for h in range(2):
            at = pl.multiple_of((2 * pair_at(q) + h) * window, window)
            rr, ri = rtr[pl.ds(at, window), :], rti[pl.ds(at, window), :]
            low = base + h * two
            wt[low : low + window, :] = (res_r * rr + res_i * ri).astype(BF)
            wt[low + window : low + two, :] = (res_i * rr - res_r * ri).astype(BF)
        grid = lax.dot_general(
            lt[...], wt[base : base + 2 * two, :], nt, preferred_element_type=F32
        )
        for g in range(groups):
            for h in range(2):
                u = grid[g * two : g * two + window, h * two : (h + 1) * two]
                v = grid[g * two + window : (g + 1) * two, h * two : (h + 1) * two]
                index = g * 8 + 2 * pair_at(q) + h
                r_send[index] = ((u + spin(v, 1.0, -1.0)) * scale).astype(BF)
        each_facet(q, send_back)
    r_recv[f] = r_send[f]
    for i in range(2 * half // 256):
        tt[:, i * 256 : (i + 1) * 256] = t2[i * 256 : (i + 1) * 256, :].T
    for q in far_first[::-1]:
        each_facet(q, take_back)

    ret = r_recv[...].reshape(half, two)
    other = spin(ret.astype(F32), 1.0, -1.0).astype(BF)

    def back_strip(cp):
        at = pl.multiple_of(cp * rows, rows)
        strip = jnp.dot(tt[pl.ds(at, rows), :half], ret, preferred_element_type=F32)
        strip += jnp.dot(tt[pl.ds(at, rows), half:], other, preferred_element_type=F32)
        b_send[cp] = strip.astype(BF)

    for step in col_steps:
        peer = col_at(step, 1)
        back_strip(peer)
        col_link(b_send, b_recv, sd, rd, peer, c).start()
    back_strip(c)
    back_out[c] = b_send[c]
    for step in col_steps[::-1]:
        src = col_at(step, -1)
        col_link(b_send, b_recv, sd, rd, src, src).wait_recv()
        back_out[src] = b_recv[src]
    for step in col_steps:
        peer = col_at(step, 1)
        col_link(s_send, s_recv, sa, ra, peer, c).wait_send()
        col_link(b_send, b_recv, sd, rd, peer, c).wait_send()
    for d in range(1, nf):
        peer = lax.rem(f + d, nf)
        facet_link(g_send, g_recv, sb, rb, peer, f).wait_send()
        facet_link(r_send, r_recv, sc, rc, peer, f).wait_send()


def image_kernel(nc, back, tab, out, buf, sem):
    tiles, tile = buf.shape[0], buf.shape[3]
    strip = jnp.concatenate([back[k] for k in range(nc)], axis=1)
    stores = []
    for t in range(tiles):
        for part in range(2):
            piece = tab[part, :, t * tile : (t + 1) * tile]
            buf[t, part] = jnp.dot(strip, piece, preferred_element_type=F32)
        store = pltpu.make_async_copy(
            buf.at[t], out.at[:, :, t * tile : (t + 1) * tile], sem.at[t]
        )
        store.start()
        stores.append(store)
    for store in stores:
        store.wait()


def solution(mesh):
    nf, nc = mesh.shape["facet"], mesh.shape["col"]

    def on_device(facets, observed, uv_cells, counts):
        rows, extent = facets.shape[1:]
        vis = observed.shape[2]
        pc = counts.shape[0]
        window = S // 8
        two = 2 * window
        groups = nf // 8
        assert pc == nf and nf % 8 == 0 and nf <= 32
        con, scal = make_constants(nf, nc, pc, extent)
        vmem = pl.BlockSpec(memory_space=pltpu.VMEM)
        smem = pl.BlockSpec(memory_space=pltpu.SMEM)
        hbm = pl.BlockSpec(memory_space=pltpu.HBM)
        dma = pltpu.SemaphoreType.DMA
        fixed = functools.partial(pltpu.with_memory_space_constraint, memory_space=pltpu.HBM)
        back, tab = pl.pallas_call(
            functools.partial(cycle_kernel, nf, nc),
            out_shape=(
                jax.ShapeDtypeStruct((nc, rows, two), BF),
                jax.ShapeDtypeStruct((2, nc * two, extent), BF),
            ),
            in_specs=[hbm, hbm, hbm, smem, hbm, smem],
            out_specs=(vmem, vmem),
            scratch_shapes=[
                pltpu.VMEM((2, rows, extent), BF),
                pltpu.VMEM((2, pc, vis), F32),
                pltpu.VMEM((2, pc, vis), jnp.int32),
                pltpu.VMEM(con.shape, F32),
                pltpu.VMEM((2 * pc * window, extent), BF),
                pltpu.VMEM((extent, 2 * pc * window), BF),
                pltpu.VMEM((nc, rows, two), BF),
                pltpu.VMEM((nc, rows, two), BF),
                pltpu.VMEM((pc, window, two), BF),
                pltpu.VMEM((nf, window, two), BF),
                pltpu.VMEM((groups * two, vis), BF),
                pltpu.VMEM((S, vis), F32),
                pltpu.VMEM((S, vis), F32),
                pltpu.VMEM((S // 16, vis), F32),
                pltpu.VMEM((S // 16, vis), F32),
                pltpu.VMEM((2 * S, vis), BF),
                pltpu.VMEM((nf, window, two), BF),
                pltpu.VMEM((pc, window, two), BF),
                pltpu.VMEM((nc, rows, two), BF),
                pltpu.VMEM((nc, rows, two), BF),
                dma((5,)),
                dma((nc,)), dma((nc,)), dma((nf,)), dma((nf,)),
                dma((nf,)), dma((nf,)), dma((nc,)), dma((nc,)),
            ],
            compiler_params=pltpu.CompilerParams(
                collective_id=0, has_side_effects=True, vmem_limit_bytes=44 * 2**20
            ),
            name="cycle",
        )(
            fixed(facets), fixed(observed), fixed(uv_cells), fixed(counts),
            fixed(jnp.asarray(con)), fixed(jnp.asarray(scal)),
        )
        tile = 256
        return pl.pallas_call(
            functools.partial(image_kernel, nc),
            out_shape=jax.ShapeDtypeStruct((2, rows, extent), F32),
            in_specs=[vmem, vmem],
            out_specs=hbm,
            scratch_shapes=[
                pltpu.VMEM((extent // tile, 2, rows, tile), F32),
                dma((extent // tile,)),
            ],
            compiler_params=pltpu.CompilerParams(vmem_limit_bytes=16 * 2**20),
            name="image",
        )(back, tab)

    return jax.shard_map(
        on_device,
        mesh=mesh,
        in_specs=(
            P(None, ("facet", "col"), None),
            P(None, "col", None),
            P(None, "col", None),
            P("col"),
        ),
        out_specs=P(None, ("facet", "col"), None),
        check_vma=False,
    )
```
